32 devices in a mesh: bar: 16 (over z, x, core), lat: 2 (over y).
Axes of the slice: x: 2, y: 2, z: 4, core: 2. Of those that a mesh axis runs over, the one named last changes fastest.
Arguments:
- displace: float32 [3, 96, 16, 128], P(None, 'bar', 'lat'), may hold values from -6 to 6
- velocity: float32 [3, 96, 16, 128], P(None, 'bar', 'lat'), may hold values from -6 to 6
- bond_low: int32 [96, 16, 128], P('bar', 'lat'), may hold values from 0 to 2147483646
- bond_high: int32 [96, 16, 128], P('bar', 'lat'), may hold values from 0 to 1073741823
- bc_type: int32 [16], replicated, may hold values from 0 to 3
Outputs:
- displace_out: float32 [3, 96, 16, 128], P(None, 'bar', 'lat')
- velocity_out: float32 [3, 96, 16, 128], P(None, 'bar', 'lat')
The draws below stay inside these ranges and needn't reach their ends.
All inputs are finite; a program needn't handle non-finite values.
Results may differ from the reference program's by a relative error of at most 0.00002.
Values sent between devices are 32-bit elements; how exact they have to be, the bound alone decides.
A program may use at most 64 MiB of HBM per device.

```python
import jax
import jax.numpy as jnp

CX = 6
STEPS = 2
NX = 96
NY = 16
NZ = 128
SLABS = 16


def plant(values, key, low, top_value):
    extent = values.shape
    place = [jax.random.randint(jax.random.fold_in(key, axis), (), 0, extent[axis]) for axis in range(len(extent))]
    values = values.at[tuple(place)].set(low)
    longest = extent.index(max(extent))
    place[longest] = (place[longest] + 1) % extent[longest]
    return values.at[tuple(place)].set(top_value)


def level_of(stream_key, dims, shards, low, largest):
    loudness = 1.0
    for axis_at, shards_of in shards:
        draws = jax.random.uniform(jax.random.fold_in(jax.random.fold_in(stream_key, 6), axis_at), (shards_of,), jnp.float32, low / len(shards), largest / len(shards))
        loudness = loudness * jnp.repeat(jnp.exp(draws), dims[axis_at] // shards_of).reshape((-1,) + (1,) * (len(dims) - 1 - axis_at))
    return loudness


def normal_values(key, dims, spread, limit, shards=(), kind=jnp.bfloat16):
    entries = spread * jax.random.normal(key, dims, jnp.float32)
    if shards:
        entries = entries * level_of(key, dims, shards, -0.22, 0.18)
    return jnp.clip(entries, -limit, limit).astype(kind)


def setup_inputs(seed: int = 0) -> dict:
    seeds = jax.random.split(jax.random.key(seed), 6)
    return {
        "displace": normal_values(seeds[0], (3, NX, NY, NZ), 1.0, 6.0, ((1, 16), (2, 2)), jnp.float32),
        "velocity": normal_values(seeds[1], (3, NX, NY, NZ), 0.5, 6.0, ((1, 16), (2, 2)), jnp.float32),
        "bond_low": plant(jax.random.randint(seeds[2], (NX, NY, NZ), 0, 2147483647), jax.random.fold_in(seeds[2], 1), 0, 2147483646).astype(jnp.int32),
        "bond_high": plant(jax.random.randint(seeds[3], (NX, NY, NZ), 0, 1073741824), jax.random.fold_in(seeds[3], 1), 0, 1073741823).astype(jnp.int32),
        "bc_type": plant(jax.random.randint(seeds[4], (SLABS,), 0, 4), jax.random.fold_in(seeds[4], 1), 0, 3).astype(jnp.int32),
    }


modulus = 0.1
time_step = 0.5


def bond_offsets():
    found = []
    for off_x in range(-3, 4):
        for off_y in range(-3, 4):
            for off_z in range(-3, 4):
                square = off_x * off_x + off_y * off_y + off_z * off_z
                if square == 0 or square > 9:
                    continue
                if off_x > 0 or (off_x == 0 and off_y > 0) or (off_x == 0 and off_y == 0 and off_z > 0):
                    found.append((off_x, off_y, off_z))
    return found


def inside(coords, shift_by, total):
    moved = coords + shift_by
    return ((moved >= 0) & (moved < total)).astype(jnp.float32)


def bond_forces(moving, low_bits, high_bits, anchor_x, anchor_y, total_x, total_y):
    size_x, size_y, size_z = moving.shape[1], moving.shape[2], moving.shape[3]
    padded = jnp.pad(moving, ((0, 0), (3, 3), (3, 3), (3, 3)))
    coord_x = anchor_x + jnp.arange(size_x, dtype=jnp.int32)
    coord_y = anchor_y + jnp.arange(size_y, dtype=jnp.int32)
    coord_z = jnp.arange(size_z, dtype=jnp.int32)
    here_x = inside(coord_x, 0, total_x)
    here_y = inside(coord_y, 0, total_y)
    force_x = jnp.zeros(moving.shape[1:], jnp.float32)
    force_y = jnp.zeros(moving.shape[1:], jnp.float32)
    force_z = jnp.zeros(moving.shape[1:], jnp.float32)
    for number, (off_x, off_y, off_z) in enumerate(bond_offsets()):
        if number < 31:
            flag_word, bit_pos = low_bits, number
        else:
            flag_word, bit_pos = high_bits, number - 31
        intact = (1 - jnp.bitwise_and(jnp.right_shift(flag_word, bit_pos), 1)).astype(jnp.float32)
        neighbour = padded[:, 3 + off_x:3 + off_x + size_x, 3 + off_y:3 + off_y + size_y, 3 + off_z:3 + off_z + size_z]
        mask_x = here_x * inside(coord_x, off_x, total_x)
        mask_y = here_y * inside(coord_y, off_y, total_y)
        mask_z = inside(coord_z, off_z, size_z)
        reach_mask = mask_x[:, None, None] * mask_y[None, :, None] * mask_z[None, None, :]
        stretch = (off_x * (neighbour[0] - moving[0]) + off_y * (neighbour[1] - moving[1])
                   + off_z * (neighbour[2] - moving[2]))
        length = float(off_x * off_x + off_y * off_y + off_z * off_z) ** 1.5
        bond_term = (modulus / length) * intact * reach_mask * stretch
        bond_pad = jnp.pad(bond_term, 3)
        back_term = bond_pad[3 - off_x:3 - off_x + size_x, 3 - off_y:3 - off_y + size_y, 3 - off_z:3 - off_z + size_z]
        net_term = bond_term - back_term
        force_x = force_x + off_x * net_term
        force_y = force_y + off_y * net_term
        force_z = force_z + off_z * net_term
    return jnp.stack([force_x, force_y, force_z])


def reference(displace, velocity, bond_low, bond_high, bc_type):
    planes = jnp.arange(NX, dtype=jnp.int32) // CX
    slabs = jnp.arange(SLABS, dtype=jnp.int32)
    match = (planes[:, None] == slabs[None, :]).astype(jnp.float32)
    code = jnp.sum(match * bc_type.astype(jnp.float32)[None, :], axis=1)
    retain = (1.0 - 0.2 * code)[None, :, None, None]
    for step_no in range(STEPS):
        forces = bond_forces(displace, bond_low, bond_high, 0, 0, NX, NY)
        velocity = retain * (velocity + time_step * forces)
        displace = displace + time_step * velocity
    return displace, velocity
```

```python
import functools

import jax
import jax.numpy as jnp
from jax import lax
from jax.experimental import pallas as pl
from jax.experimental.pallas import tpu as pltpu
from jax.sharding import PartitionSpec as P

STEPS = 2
REACH = 3
MODULUS = 0.1
TIME_STEP = 0.5
WORD = 31
MESH = pl.DeviceIdType.MESH
ROW = 8


def bond_offsets():
    found = []
    for a in range(-REACH, REACH + 1):
        for b in range(-REACH, REACH + 1):
            for c in range(-REACH, REACH + 1):
                square = a * a + b * b + c * c
                if 0 < square <= REACH * REACH and (a, b, c) > (0, 0, 0):
                    found.append((a, b, c))
    return found


BONDS = {offset: number for number, offset in enumerate(bond_offsets())}
DIRECTED = {}
for _offset, _number in BONDS.items():
    DIRECTED[_offset] = (_number, True)
    DIRECTED[tuple(-v for v in _offset)] = (_number, False)
COLUMNS = sorted({(b, c) for _, b, c in DIRECTED}, key=lambda bc: (abs(bc[0]), bc))
ALONG = {bc: sorted(a for a, b, c in DIRECTED if (b, c) == bc) for bc in COLUMNS}
SLOT = {offset: place for place, offset in enumerate(sorted(DIRECTED))}


def word_bits(test):
    words = [0, 0]
    for offset, number in BONDS.items():
        if test(offset):
            words[number // WORD] |= 1 << (number % WORD)
    return words


def times(factor, value):
    if factor == 1:
        return value
    if factor == -1:
        return -value
    return float(factor) * value


def plus_times(total, factor, value):
    if factor == 0:
        return total
    if total is None:
        return times(factor, value)
    if factor == 1:
        return total + value
    if factor == -1:
        return total - value
    return total + float(factor) * value


def add_planes(total, start, value):
    count = total.shape[0]
    stop = start + value.shape[0]
    parts = []
    if start > 0:
        parts.append(total[:start])
    parts.append(total[start:stop] + value)
    if stop < count:
        parts.append(total[stop:])
    return parts[0] if len(parts) == 1 else jnp.concatenate(parts, axis=0)


def kernel(
    n_bar,
    n_lat,
    u_ref,
    v_ref,
    low_ref,
    high_ref,
    bc_ref,
    uo_ref,
    vo_ref,
    u_mid,
    field,
    flags,
    weight,
    pack_lat,
    pack_corner,
    pack_flag_lat,
    pack_flag_corner,
    got_bar,
    got_lat,
    got_corner,
    got_high,
    got_low,
    got_flag_lat,
    got_flag_corner,
    send_sem,
    recv_sem,
):
    size_x, size_y, size_z = u_ref.shape[1:]
    me_bar = lax.axis_index("bar")
    me_lat = lax.axis_index("lat")

    def there(d_bar, d_lat):
        ok = None
        for step, me, count in ((d_bar, me_bar, n_bar), (d_lat, me_lat, n_lat)):
            if step:
                good = me > 0 if step < 0 else me < count - 1
                ok = good if ok is None else jnp.logical_and(ok, good)
        return ok

    around = [(i, j) for i in (-1, 0, 1) for j in (-1, 0, 1) if (i, j) != (0, 0)]
    barrier = pltpu.get_barrier_semaphore()
    for i, j in around:

        @pl.when(there(i, j))
        def _():
            pl.semaphore_signal(barrier, inc=1, device_id=(me_bar + i, me_lat + j), device_id_type=MESH)

    def rows_of(side, width):
        return slice(0, width) if side == 0 else slice(size_y - width, size_y)

    def pack_moving(step, source):
        for side in range(2):
            for comp in range(3):
                for p in range(size_x):
                    at = (comp * size_x + p) * 3
                    pack_lat[step, side, at : at + 3, :] = source[comp, p, rows_of(side, 3), :]
                for end in range(2):
                    for q in range(2):
                        p = q if end == 0 else size_x - 2 + q
                        at = (comp * 2 + q) * 2
                        pack_corner[step, end, side, at : at + 2, :] = source[comp, p, rows_of(side, 2), :]

    words = (low_ref, high_ref)
    for side in range(2):
        for w in range(2):
            for p in range(size_x):
                at = (w * size_x + p) * 3
                pack_flag_lat[side, at : at + 3, :] = words[w][p, rows_of(side, 3), :]
        for at, (w, p) in enumerate(((0, size_x - 1), (1, size_x - 2), (1, size_x - 1))):
            pack_flag_corner[side, 2 * at : 2 * at + 2, :] = words[w][p, rows_of(side, 2), :]
    pack_moving(0, u_ref)

    for end in range(2):

        @pl.when(jnp.logical_not(there(2 * end - 1, 0)))
        def _():
            for step in range(STEPS):
                got_bar[step, end] = jnp.zeros(got_bar.shape[2:], jnp.float32)

        @pl.when(jnp.logical_not(there(0, 2 * end - 1)))
        def _():
            for step in range(STEPS):
                got_lat[step, end] = jnp.zeros(got_lat.shape[2:], jnp.float32)
            got_flag_lat[end] = jnp.full(got_flag_lat.shape[1:], -1, jnp.int32)

        for side in range(2):

            @pl.when(jnp.logical_not(there(2 * end - 1, 2 * side - 1)))
            def _():
                for step in range(STEPS):
                    got_corner[step, end, side] = jnp.zeros(got_corner.shape[3:], jnp.float32)
                if end == 0:
                    got_flag_corner[side] = jnp.full(got_flag_corner.shape[1:], -1, jnp.int32)

    @pl.when(jnp.logical_not(there(-1, 0)))
    def _():
        got_high[...] = jnp.full(got_high.shape, -1, jnp.int32)
        got_low[...] = jnp.full(got_low.shape, -1, jnp.int32)

    copies = []

    def post(group, source, target, i, j):
        place = len(copies)
        copy = pltpu.make_async_remote_copy(
            src_ref=source,
            dst_ref=target,
            send_sem=send_sem.at[place],
            recv_sem=recv_sem.at[place],
            device_id=(me_bar + i, me_lat + j),
            device_id_type=MESH,
        )

        @pl.when(there(i, j))
        def _():
            copy.start()

        copies.append((group, copy, (i, j)))

    def send_moving(step, source):
        for side in range(2):
            post((step, "lat"), pack_lat.at[step, side], got_lat.at[step, 1 - side], 0, 2 * side - 1)
        for end in range(2):
            first = 0 if end == 0 else size_x - 3
            post((step, "bar"), source.at[:, first : first + 3], got_bar.at[step, 1 - end], 2 * end - 1, 0)
            for side in range(2):
                post(
                    (step, "bar"),
                    pack_corner.at[step, end, side],
                    got_corner.at[step, 1 - end, 1 - side],
                    2 * end - 1,
                    2 * side - 1,
                )

    def wait(group):
        for name, copy, (i, j) in copies:
            if name == group:

                @pl.when(there(-i, -j))
                def _():
                    copy.wait_recv()

    span_bar = (me_bar > 0).astype(jnp.int32) + (me_bar < n_bar - 1).astype(jnp.int32)
    span_lat = (me_lat > 0).astype(jnp.int32) + (me_lat < n_lat - 1).astype(jnp.int32)
    pl.semaphore_wait(barrier, (span_bar + 1) * (span_lat + 1) - 1)

    for side in range(2):
        post((0, "lat"), pack_flag_lat.at[side], got_flag_lat.at[1 - side], 0, 2 * side - 1)
    post((0, "bar"), high_ref.at[size_x - 3 :], got_high, 1, 0)
    post((0, "bar"), low_ref.at[size_x - 1 :], got_low, 1, 0)
    for side in range(2):
        post((0, "bar"), pack_flag_corner.at[side], got_flag_corner.at[1 - side], 1, 2 * side - 1)
    send_moving(0, u_ref)

    lane = lax.broadcasted_iota(jnp.int32, (size_y, size_z), 1)
    row = lax.broadcasted_iota(jnp.int32, (size_y, size_z), 0) + me_lat * size_y
    zero = jnp.zeros((size_y, size_z), jnp.int32)
    leave_z, leave_y = [zero, zero], [zero, zero]
    for d in (-3, -2, -1, 1, 2, 3):
        bits = word_bits(lambda o: o[2] == d)
        gone = (lane + d < 0) | (lane + d >= size_z)
        leave_z = [m | jnp.where(gone, x, 0) for m, x in zip(leave_z, bits)]
        bits = word_bits(lambda o: o[1] == d)
        gone = (row + d < 0) | (row + d >= size_y * n_lat)
        leave_y = [m | jnp.where(gone, x, 0) for m, x in zip(leave_y, bits)]
    last = me_bar == n_bar - 1

    def rolled(value, c):
        return value if c == 0 else pltpu.roll(value, (-c) % size_z, axis=value.ndim - 1)

    def fill_rows(buffer, lead, value, c):
        buffer[(c + 3,) + lead + (slice(ROW, ROW + size_y),)] = rolled(value, c)

    def fill_halo(buffer, lead, value, c):
        moved = rolled(value, c)
        buffer[(c + 3,) + lead + (slice(0, ROW),)] = moved
        buffer[(c + 3,) + lead + (slice(ROW + size_y, 2 * ROW + size_y),)] = moved

    def halo_of(buffer, lead):
        return buffer[(3,) + lead + (slice(0, ROW),)]

    for w in range(2):
        for p in range(size_x):
            leave_x = word_bits(lambda o: o[0] + p >= size_x)[w]
            word = words[w][p] | leave_z[w] | leave_y[w] | jnp.where(last, leave_x, 0)
            for c in range(-3, 4):
                fill_rows(flags, (w, 3 + p), word, c)

    planes = slice(3, 3 + size_x)

    def fill_own(source):
        for comp in range(3):
            value = source[comp]
            for c in range(-3, 4):
                fill_rows(field, (comp, planes), value, c)

    def flag_at(c, w, lead, rows):
        return flags[c + 3, w, lead, rows, :]

    def weights(step, offset, start, stop):
        place = SLOT[offset]
        if step > 0:
            return weight[place, start:stop]
        number, forward = DIRECTED[offset]
        a, b, c = offset
        w, bit = number // WORD, 1 << (number % WORD)
        if forward:
            word = flags[3, w, 3 + start : 3 + stop, ROW : ROW + size_y, :]
        else:
            word = flags[c + 3, w, 3 + start + a : 3 + stop + a, ROW + b : ROW + b + size_y, :]
        value = MODULUS / float(a * a + b * b + c * c) ** 1.5
        found = jnp.where((word & bit) == 0, jnp.float32(value), jnp.float32(0.0))
        weight[place, start:stop] = found
        return found

    def near(comp, b, c, start, stop):
        return field[c + 3, comp, 3 + start : 3 + stop, ROW + b : ROW + b + size_y, :]

    def inner(step, columns, force):
        for b, c in columns:
            mine, other = None, None
            for comp, factor in ((1, b), (2, c)):
                if factor:
                    mine = plus_times(mine, factor, near(comp, 0, 0, 0, size_x))
                    other = plus_times(other, factor, near(comp, b, c, 0, size_x))
            mine_x = near(0, 0, 0, 0, size_x)
            other_x = near(0, b, c, 0, size_x)
            total, total_x = None, None
            for a in sorted(ALONG[b, c], key=abs):
                start, stop = max(0, -a), min(size_x, size_x - a)
                if mine is None:
                    stretch = times(a, other_x[start + a : stop + a] - mine_x[start:stop])
                else:
                    stretch = plus_times(other[start + a : stop + a], a, other_x[start + a : stop + a])
                    stretch = stretch - plus_times(mine[start:stop], a, mine_x[start:stop])
                term = weights(step, (a, b, c), start, stop) * stretch
                if mine is not None:
                    total = term if total is None else add_planes(total, start, term)
                if a:
                    if total_x is None:
                        total_x = jnp.zeros((size_x, size_y, size_z), jnp.float32)
                    total_x = add_planes(total_x, start, times(a, term))
            if total_x is not None:
                force[0] = force[0] + total_x
            for comp, factor in ((1, b), (2, c)):
                force[comp] = plus_times(force[comp], factor, total) if factor else force[comp]

    def outer(step, force):
        for b, c in COLUMNS:
            for end in range(2):
                for a in ALONG[b, c]:
                    if a == 0 or (a > 0) != (end == 1):
                        continue
                    start, stop = (0, -a) if a < 0 else (size_x - a, size_x)
                    stretch = None
                    for comp, factor in ((0, a), (1, b), (2, c)):
                        if factor:
                            change = near(comp, b, c, start + a, stop + a) - near(comp, 0, 0, start, stop)
                            stretch = plus_times(stretch, factor, change)
                    term = weights(step, (a, b, c), start, stop) * stretch
                    for comp, factor in ((0, a), (1, b), (2, c)):
                        if factor:
                            force[comp] = add_planes(force[comp], start, times(factor, term))

    code = bc_ref[me_bar].astype(jnp.float32)
    retain = 1.0 - 0.2 * code

    flat = [bc for bc in COLUMNS if bc[0] == 0]
    tilted = [bc for bc in COLUMNS if bc[0] != 0]
    for step in range(STEPS):
        source = u_ref if step == 0 else u_mid
        old_v = v_ref if step == 0 else vo_ref
        fill_own(source)
        force = [jnp.zeros((size_x, size_y, size_z), jnp.float32)] * 3
        inner(step, flat, force)

        wait((step, "lat"))
        if step == 0:
            for w in range(2):
                for p in range(size_x):
                    at = (w * size_x + p) * 3
                    flags[3, w, 3 + p, ROW - 3 : ROW, :] = got_flag_lat[0, at : at + 3, :]
                    flags[3, w, 3 + p, 0:3, :] = got_flag_lat[1, at : at + 3, :]
                    value = halo_of(flags, (w, 3 + p)) | leave_z[w]
                    for c in range(-2, 3):
                        fill_halo(flags, (w, 3 + p), value, c)
        for comp in range(3):
            for p in range(size_x):
                at = (comp * size_x + p) * 3
                field[3, comp, 3 + p, ROW - 3 : ROW, :] = got_lat[step, 0, at : at + 3, :]
                field[3, comp, 3 + p, 0:3, :] = got_lat[step, 1, at : at + 3, :]
            value = halo_of(field, (comp, planes))
            for c in range(-2, 3):
                fill_halo(field, (comp, planes), value, c)
        inner(step, tilted, force)

        wait((step, "bar"))
        if step == 0:
            for at, (w, q) in enumerate(((0, 2), (1, 1), (1, 2))):
                flags[3, w, q, ROW - 2 : ROW, :] = got_flag_corner[0, 2 * at : 2 * at + 2, :]
                flags[3, w, q, 0:2, :] = got_flag_corner[1, 2 * at : 2 * at + 2, :]
                own = got_low[0] if w == 0 else got_high[q]
                own = own | leave_z[w]
                value = halo_of(flags, (w, q)) | leave_z[w]
                for c in range(-2, 3):
                    fill_rows(flags, (w, q), own, c)
                    fill_halo(flags, (w, q), value, c)
            fill_rows(flags, (1, 0), got_high[0], 0)
        for comp in range(3):
            for end in range(2):
                first = 1 if end == 0 else 3 + size_x
                for q in range(2):
                    at = (comp * 2 + q) * 2
                    field[3, comp, first + q, ROW - 2 : ROW, :] = got_corner[step, end, 0, at : at + 2, :]
                    field[3, comp, first + q, 0:2, :] = got_corner[step, end, 1, at : at + 2, :]
                lead = (comp, slice(first, first + 2))
                value = halo_of(field, lead)
                own = got_bar[step, end, comp, 1 - end : 3 - end]
                for c in range(-2, 3):
                    fill_halo(field, lead, value, c)
                    fill_rows(field, lead, own, c)
                far = 0 if end == 0 else 5 + size_x
                fill_rows(field, (comp, far), got_bar[step, end, comp, 2 * end], 0)
        outer(step, force)

        for comp in range(3):
            fast = retain * (old_v[comp] + TIME_STEP * force[comp])
            moved = source[comp] + TIME_STEP * fast
            vo_ref[comp] = fast
            if step == STEPS - 1:
                uo_ref[comp] = moved
            else:
                u_mid[comp] = moved
        if step < STEPS - 1:
            pack_moving(step + 1, u_mid)
            send_moving(step + 1, u_mid)

    for _, copy, (i, j) in copies:

        @pl.when(there(i, j))
        def _():
            copy.wait_send()


def local(n_bar, n_lat, displace, velocity, bond_low, bond_high, bc_type):
    _, size_x, size_y, size_z = displace.shape

    def up(rows):
        return -(-rows // 8) * 8

    rows_lat, rows_corner, rows_flag = up(9 * size_x), up(12), up(6 * size_x)
    copies = 6 + 8 * STEPS
    vmem = pl.BlockSpec(memory_space=pltpu.VMEM)
    return pl.pallas_call(
        functools.partial(kernel, n_bar, n_lat),
        out_shape=(
            jax.ShapeDtypeStruct(displace.shape, jnp.float32),
            jax.ShapeDtypeStruct(velocity.shape, jnp.float32),
        ),
        in_specs=[vmem] * 4 + [pl.BlockSpec(memory_space=pltpu.SMEM)],
        out_specs=(vmem, vmem),
        scratch_shapes=[
            pltpu.VMEM(displace.shape, jnp.float32),
            pltpu.VMEM((7, 3, size_x + 6, size_y + 16, size_z), jnp.float32),
            pltpu.VMEM((7, 2, size_x + 3, size_y + 16, size_z), jnp.int32),
            pltpu.VMEM((len(DIRECTED), size_x, size_y, size_z), jnp.float32),
            pltpu.VMEM((STEPS, 2, rows_lat, size_z), jnp.float32),
            pltpu.VMEM((STEPS, 2, 2, rows_corner, size_z), jnp.float32),
            pltpu.VMEM((2, rows_flag, size_z), jnp.int32),
            pltpu.VMEM((2, 8, size_z), jnp.int32),
            pltpu.VMEM((STEPS, 2, 3, 3, size_y, size_z), jnp.float32),
            pltpu.VMEM((STEPS, 2, rows_lat, size_z), jnp.float32),
            pltpu.VMEM((STEPS, 2, 2, rows_corner, size_z), jnp.float32),
            pltpu.VMEM((3, size_y, size_z), jnp.int32),
            pltpu.VMEM((1, size_y, size_z), jnp.int32),
            pltpu.VMEM((2, rows_flag, size_z), jnp.int32),
            pltpu.VMEM((2, 8, size_z), jnp.int32),
            pltpu.SemaphoreType.DMA((copies,)),
            pltpu.SemaphoreType.DMA((copies,)),
        ],
        compiler_params=pltpu.CompilerParams(collective_id=0, has_side_effects=True),
        name="leapfrog",
    )(displace, velocity, bond_low, bond_high, bc_type)


def solution(mesh):
    cells = P(None, "bar", "lat", None)
    return jax.shard_map(
        functools.partial(local, mesh.shape["bar"], mesh.shape["lat"]),
        mesh=mesh,
        in_specs=(cells, cells, P("bar", "lat", None), P("bar", "lat", None), P()),
        out_specs=(cells, cells),
        check_vma=False,
    )
```

```python
import functools

import jax
import jax.numpy as jnp
from jax import lax
from jax.experimental import pallas as pl
from jax.experimental.pallas import tpu as pltpu
from jax.sharding import PartitionSpec as P

STEPS = 2
REACH = 3
MODULUS = 0.1
TIME_STEP = 0.5
WORD = 31
MESH = pl.DeviceIdType.MESH
ROW = 8


def bond_offsets():
    found = []
    for a in range(-REACH, REACH + 1):
        for b in range(-REACH, REACH + 1):
            for c in range(-REACH, REACH + 1):
                square = a * a + b * b + c * c
                if 0 < square <= REACH * REACH and (a, b, c) > (0, 0, 0):
                    found.append((a, b, c))
    return found


BONDS = {offset: number for number, offset in enumerate(bond_offsets())}
DIRECTED = {}
for _offset, _number in BONDS.items():
    DIRECTED[_offset] = (_number, True)
    DIRECTED[tuple(-v for v in _offset)] = (_number, False)
COLUMNS = sorted({(b, c) for _, b, c in DIRECTED}, key=lambda bc: (abs(bc[0]), bc))
ALONG = {bc: sorted(a for a, b, c in DIRECTED if (b, c) == bc) for bc in COLUMNS}
SLOT = {offset: place for place, offset in enumerate(sorted(DIRECTED))}


def word_bits(test):
    words = [0, 0]
    for offset, number in BONDS.items():
        if test(offset):
            words[number // WORD] |= 1 << (number % WORD)
    return words


def times(factor, value):
    if factor == 1:
        return value
    if factor == -1:
        return -value
    return float(factor) * value


def plus_times(total, factor, value):
    if factor == 0:
        return total
    if total is None:
        return times(factor, value)
    if factor == 1:
        return total + value
    if factor == -1:
        return total - value
    return total + float(factor) * value


def add_planes(total, start, value):
    count = total.shape[0]
    stop = start + value.shape[0]
    parts = []
    if start > 0:
        parts.append(total[:start])
    parts.append(total[start:stop] + value)
    if stop < count:
        parts.append(total[stop:])
    return parts[0] if len(parts) == 1 else jnp.concatenate(parts, axis=0)


def kernel(
    n_bar,
    n_lat,
    u_in,
    v_in,
    low_in,
    high_in,
    bc_ref,
    u_mid_out,
    vo_ref,
    u_ref,
    v_ref,
    low_ref,
    high_ref,
    u_mid,
    field,
    flags,
    weight,
    pack_lat,
    pack_corner,
    pack_flag_lat,
    pack_flag_corner,
    got_bar,
    got_lat,
    got_corner,
    got_high,
    got_low,
    got_flag_lat,
    got_flag_corner,
    send_sem,
    recv_sem,
    load_sem,
):
    size_x, size_y, size_z = u_ref.shape[1:]
    me_bar = lax.axis_index("bar")
    me_lat = lax.axis_index("lat")

    def there(d_bar, d_lat):
        ok = None
        for step, me, count in ((d_bar, me_bar, n_bar), (d_lat, me_lat, n_lat)):
            if step:
                good = me > 0 if step < 0 else me < count - 1
                ok = good if ok is None else jnp.logical_and(ok, good)
        return ok

    around = [(i, j) for i in (-1, 0, 1) for j in (-1, 0, 1) if (i, j) != (0, 0)]
    barrier = pltpu.get_barrier_semaphore()
    for i, j in around:

        @pl.when(there(i, j))
        def _():
            pl.semaphore_signal(barrier, inc=1, device_id=(me_bar + i, me_lat + j), device_id_type=MESH)

    loads = [
        pltpu.make_async_copy(source, target, load_sem.at[place])
        for place, (source, target) in enumerate(
            ((u_in, u_ref), (low_in, low_ref), (high_in, high_ref), (v_in, v_ref))
        )
    ]
    for load in loads:
        load.start()

    def rows_of(side, width):
        return slice(0, width) if side == 0 else slice(size_y - width, size_y)

    def pack_moving(step, source):
        for side in range(2):
            for comp in range(3):
                for p in range(size_x):
                    at = (comp * size_x + p) * 3
                    pack_lat[step, side, at : at + 3, :] = source[comp, p, rows_of(side, 3), :]
                for end in range(2):
                    for q in range(2):
                        p = q if end == 0 else size_x - 2 + q
                        at = (comp * 2 + q) * 2
                        pack_corner[step, end, side, at : at + 2, :] = source[comp, p, rows_of(side, 2), :]

    for end in range(2):

        @pl.when(jnp.logical_not(there(2 * end - 1, 0)))
        def _():
            for step in range(STEPS):
                got_bar[step, end] = jnp.zeros(got_bar.shape[2:], jnp.float32)

        @pl.when(jnp.logical_not(there(0, 2 * end - 1)))
        def _():
            for step in range(STEPS):
                got_lat[step, end] = jnp.zeros(got_lat.shape[2:], jnp.float32)
            got_flag_lat[end] = jnp.full(got_flag_lat.shape[1:], -1, jnp.int32)

        for side in range(2):

            @pl.when(jnp.logical_not(there(2 * end - 1, 2 * side - 1)))
            def _():
                for step in range(STEPS):
                    got_corner[step, end, side] = jnp.zeros(got_corner.shape[3:], jnp.float32)
                if end == 0:
                    got_flag_corner[side] = jnp.full(got_flag_corner.shape[1:], -1, jnp.int32)

    @pl.when(jnp.logical_not(there(-1, 0)))
    def _():
        got_high[...] = jnp.full(got_high.shape, -1, jnp.int32)
        got_low[...] = jnp.full(got_low.shape, -1, jnp.int32)

    for load in loads[:3]:
        load.wait()
    pack_moving(0, u_ref)
    words = (low_ref, high_ref)
    for side in range(2):
        for w in range(2):
            for p in range(size_x):
                at = (w * size_x + p) * 3
                pack_flag_lat[side, at : at + 3, :] = words[w][p, rows_of(side, 3), :]
        for at, (w, p) in enumerate(((0, size_x - 1), (1, size_x - 2), (1, size_x - 1))):
            pack_flag_corner[side, 2 * at : 2 * at + 2, :] = words[w][p, rows_of(side, 2), :]

    copies = []

    def post(group, source, target, i, j):
        place = len(copies)
        copy = pltpu.make_async_remote_copy(
            src_ref=source,
            dst_ref=target,
            send_sem=send_sem.at[place],
            recv_sem=recv_sem.at[place],
            device_id=(me_bar + i, me_lat + j),
            device_id_type=MESH,
        )

        @pl.when(there(i, j))
        def _():
            copy.start()

        copies.append((group, copy, (i, j)))

    def send_moving(step, source):
        for end in range(2):
            for side in range(2):
                post(
                    (step, "bar"),
                    pack_corner.at[step, end, side],
                    got_corner.at[step, 1 - end, 1 - side],
                    2 * end - 1,
                    2 * side - 1,
                )
        if step == 0:
            for side in range(2):
                post((0, "bar"), pack_flag_corner.at[side], got_flag_corner.at[1 - side], 1, 2 * side - 1)
        for side in range(2):
            post((step, "lat"), pack_lat.at[step, side], got_lat.at[step, 1 - side], 0, 2 * side - 1)
        for end in range(2):
            first = 0 if end == 0 else size_x - 3
            post((step, "bar"), source.at[:, first : first + 3], got_bar.at[step, 1 - end], 2 * end - 1, 0)
        if step == 0:
            for side in range(2):
                post((0, "lat"), pack_flag_lat.at[side], got_flag_lat.at[1 - side], 0, 2 * side - 1)
            post((0, "bar"), high_ref.at[size_x - 3 :], got_high, 1, 0)
            post((0, "bar"), low_ref.at[size_x - 1 :], got_low, 1, 0)

    def wait(group):
        for name, copy, (i, j) in copies:
            if name == group:

                @pl.when(there(-i, -j))
                def _():
                    copy.wait_recv()

    span_bar = (me_bar > 0).astype(jnp.int32) + (me_bar < n_bar - 1).astype(jnp.int32)
    span_lat = (me_lat > 0).astype(jnp.int32) + (me_lat < n_lat - 1).astype(jnp.int32)
    pl.semaphore_wait(barrier, (span_bar + 1) * (span_lat + 1) - 1)

    send_moving(0, u_ref)

    lane = lax.broadcasted_iota(jnp.int32, (size_y, size_z), 1)
    row = lax.broadcasted_iota(jnp.int32, (size_y, size_z), 0) + me_lat * size_y
    zero = jnp.zeros((size_y, size_z), jnp.int32)
    leave_z, leave_y = [zero, zero], [zero, zero]
    for d in (-3, -2, -1, 1, 2, 3):
        bits = word_bits(lambda o: o[2] == d)
        gone = (lane + d < 0) | (lane + d >= size_z)
        leave_z = [m | jnp.where(gone, x, 0) for m, x in zip(leave_z, bits)]
        bits = word_bits(lambda o: o[1] == d)
        gone = (row + d < 0) | (row + d >= size_y * n_lat)
        leave_y = [m | jnp.where(gone, x, 0) for m, x in zip(leave_y, bits)]
    last = me_bar == n_bar - 1

    def rolled(value, c):
        return value if c == 0 else pltpu.roll(value, (-c) % size_z, axis=value.ndim - 1)

    def fill_rows(buffer, lead, value, c):
        buffer[(c + 3,) + lead + (slice(ROW, ROW + size_y),)] = rolled(value, c)

    def fill_halo(buffer, lead, value, c):
        moved = rolled(value, c)
        buffer[(c + 3,) + lead + (slice(0, ROW),)] = moved
        buffer[(c + 3,) + lead + (slice(ROW + size_y, 2 * ROW + size_y),)] = moved

    def halo_of(buffer, lead):
        return buffer[(3,) + lead + (slice(0, ROW),)]

    for w in range(2):
        for p in range(size_x):
            leave_x = word_bits(lambda o: o[0] + p >= size_x)[w]
            word = words[w][p] | leave_z[w] | leave_y[w] | jnp.where(last, leave_x, 0)
            for c in range(-3, 4):
                fill_rows(flags, (w, 3 + p), word, c)

    planes = slice(3, 3 + size_x)

    def fill_own(source):
        for comp in range(3):
            value = source[comp]
            for c in range(-3, 4):
                fill_rows(field, (comp, planes), value, c)

    def flag_at(c, w, lead, rows):
        return flags[c + 3, w, lead, rows, :]

    def weights(step, offset, start, stop):
        place = SLOT[offset]
        if step > 0:
            return weight[place, start:stop]
        number, forward = DIRECTED[offset]
        a, b, c = offset
        w, bit = number // WORD, 1 << (number % WORD)
        if forward:
            word = flags[3, w, 3 + start : 3 + stop, ROW : ROW + size_y, :]
        else:
            word = flags[c + 3, w, 3 + start + a : 3 + stop + a, ROW + b : ROW + b + size_y, :]
        value = MODULUS / float(a * a + b * b + c * c) ** 1.5
        found = jnp.where((word & bit) == 0, jnp.float32(value), jnp.float32(0.0))
        weight[place, start:stop] = found
        return found

    def near(comp, b, c, start, stop):
        return field[c + 3, comp, 3 + start : 3 + stop, ROW + b : ROW + b + size_y, :]

    def inner(step, columns, force):
        for b, c in columns:
            mine, other = None, None
            for comp, factor in ((1, b), (2, c)):
                if factor:
                    mine = plus_times(mine, factor, near(comp, 0, 0, 0, size_x))
                    other = plus_times(other, factor, near(comp, b, c, 0, size_x))
            mine_x = near(0, 0, 0, 0, size_x)
            other_x = near(0, b, c, 0, size_x)
            total, total_x = None, None
            for a in sorted(ALONG[b, c], key=abs):
                start, stop = max(0, -a), min(size_x, size_x - a)
                if mine is None:
                    stretch = times(a, other_x[start + a : stop + a] - mine_x[start:stop])
                else:
                    stretch = plus_times(other[start + a : stop + a], a, other_x[start + a : stop + a])
                    stretch = stretch - plus_times(mine[start:stop], a, mine_x[start:stop])
                term = weights(step, (a, b, c), start, stop) * stretch
                if mine is not None:
                    total = term if total is None else add_planes(total, start, term)
                if a:
                    if total_x is None:
                        total_x = jnp.zeros((size_x, size_y, size_z), jnp.float32)
                    total_x = add_planes(total_x, start, times(a, term))
            if total_x is not None:
                force[0] = force[0] + total_x
            for comp, factor in ((1, b), (2, c)):
                force[comp] = plus_times(force[comp], factor, total) if factor else force[comp]

    def outer(step, force):
        for b, c in COLUMNS:
            for end in range(2):
                for a in ALONG[b, c]:
                    if a == 0 or (a > 0) != (end == 1):
                        continue
                    start, stop = (0, -a) if a < 0 else (size_x - a, size_x)
                    stretch = None
                    for comp, factor in ((0, a), (1, b), (2, c)):
                        if factor:
                            change = near(comp, b, c, start + a, stop + a) - near(comp, 0, 0, start, stop)
                            stretch = plus_times(stretch, factor, change)
                    term = weights(step, (a, b, c), start, stop) * stretch
                    for comp, factor in ((0, a), (1, b), (2, c)):
                        if factor:
                            force[comp] = add_planes(force[comp], start, times(factor, term))

    code = bc_ref[me_bar].astype(jnp.float32)
    retain = 1.0 - 0.2 * code

    flat = [bc for bc in COLUMNS if bc[0] == 0]
    tilted = [bc for bc in COLUMNS if bc[0] != 0]
    for step in range(STEPS):
        source = u_ref if step == 0 else u_mid
        old_v = v_ref if step == 0 else vo_ref
        fill_own(source)
        force = [jnp.zeros((size_x, size_y, size_z), jnp.float32)] * 3
        inner(step, flat, force)

        wait((step, "lat"))
        if step == 0:
            for w in range(2):
                for p in range(size_x):
                    at = (w * size_x + p) * 3
                    flags[3, w, 3 + p, ROW - 3 : ROW, :] = got_flag_lat[0, at : at + 3, :]
                    flags[3, w, 3 + p, 0:3, :] = got_flag_lat[1, at : at + 3, :]
                    value = halo_of(flags, (w, 3 + p)) | leave_z[w]
                    for c in range(-2, 3):
                        fill_halo(flags, (w, 3 + p), value, c)
        for comp in range(3):
            for p in range(size_x):
                at = (comp * size_x + p) * 3
                field[3, comp, 3 + p, ROW - 3 : ROW, :] = got_lat[step, 0, at : at + 3, :]
                field[3, comp, 3 + p, 0:3, :] = got_lat[step, 1, at : at + 3, :]
            value = halo_of(field, (comp, planes))
            for c in range(-2, 3):
                fill_halo(field, (comp, planes), value, c)
        inner(step, tilted, force)

        wait((step, "bar"))
        if step == 0:
            for at, (w, q) in enumerate(((0, 2), (1, 1), (1, 2))):
                flags[3, w, q, ROW - 2 : ROW, :] = got_flag_corner[0, 2 * at : 2 * at + 2, :]
                flags[3, w, q, 0:2, :] = got_flag_corner[1, 2 * at : 2 * at + 2, :]
                own = got_low[0] if w == 0 else got_high[q]
                own = own | leave_z[w]
                value = halo_of(flags, (w, q)) | leave_z[w]
                for c in range(-2, 3):
                    fill_rows(flags, (w, q), own, c)
                    fill_halo(flags, (w, q), value, c)
            fill_rows(flags, (1, 0), got_high[0], 0)
        for comp in range(3):
            for end in range(2):
                first = 1 if end == 0 else 3 + size_x
                for q in range(2):
                    at = (comp * 2 + q) * 2
                    field[3, comp, first + q, ROW - 2 : ROW, :] = got_corner[step, end, 0, at : at + 2, :]
                    field[3, comp, first + q, 0:2, :] = got_corner[step, end, 1, at : at + 2, :]
                lead = (comp, slice(first, first + 2))
                value = halo_of(field, lead)
                own = got_bar[step, end, comp, 1 - end : 3 - end]
                for c in range(-2, 3):
                    fill_halo(field, lead, value, c)
                    fill_rows(field, lead, own, c)
                far = 0 if end == 0 else 5 + size_x
                fill_rows(field, (comp, far), got_bar[step, end, comp, 2 * end], 0)
        outer(step, force)

        for comp in range(3):
            if step == 0 and comp == 0:
                loads[3].wait()
            fast = retain * (old_v[comp] + TIME_STEP * force[comp])
            vo_ref[comp] = fast
            if step == STEPS - 1:
                u_mid_out[comp] = source[comp]
            else:
                u_mid[comp] = source[comp] + TIME_STEP * fast
        if step < STEPS - 1:
            pack_moving(step + 1, u_mid)
            send_moving(step + 1, u_mid)

    for _, copy, (i, j) in copies:

        @pl.when(there(i, j))
        def _():
            copy.wait_send()


def advance(u_ref, v_ref, uo_ref, vo_ref):
    fast = v_ref[...]
    uo_ref[...] = u_ref[...] + TIME_STEP * fast
    vo_ref[...] = fast


def local(n_bar, n_lat, displace, velocity, bond_low, bond_high, bc_type):
    _, size_x, size_y, size_z = displace.shape

    def up(rows):
        return -(-rows // 8) * 8

    rows_lat, rows_corner, rows_flag = up(9 * size_x), up(12), up(6 * size_x)
    copies = 6 + 8 * STEPS
    vmem = pl.BlockSpec(memory_space=pltpu.VMEM)
    out_shape = (
        jax.ShapeDtypeStruct(displace.shape, jnp.float32),
        jax.ShapeDtypeStruct(velocity.shape, jnp.float32),
    )
    moved, fast = pl.pallas_call(
        functools.partial(kernel, n_bar, n_lat),
        out_shape=out_shape,
        in_specs=[pl.BlockSpec(memory_space=pl.ANY)] * 4 + [pl.BlockSpec(memory_space=pltpu.SMEM)],
        out_specs=(vmem, vmem),
        scratch_shapes=[
            pltpu.VMEM(displace.shape, jnp.float32),
            pltpu.VMEM(velocity.shape, jnp.float32),
            pltpu.VMEM(bond_low.shape, jnp.int32),
            pltpu.VMEM(bond_high.shape, jnp.int32),
            pltpu.VMEM(displace.shape, jnp.float32),
            pltpu.VMEM((7, 3, size_x + 6, size_y + 16, size_z), jnp.float32),
            pltpu.VMEM((7, 2, size_x + 3, size_y + 16, size_z), jnp.int32),
            pltpu.VMEM((len(DIRECTED), size_x, size_y, size_z), jnp.float32),
            pltpu.VMEM((STEPS, 2, rows_lat, size_z), jnp.float32),
            pltpu.VMEM((STEPS, 2, 2, rows_corner, size_z), jnp.float32),
            pltpu.VMEM((2, rows_flag, size_z), jnp.int32),
            pltpu.VMEM((2, 8, size_z), jnp.int32),
            pltpu.VMEM((STEPS, 2, 3, 3, size_y, size_z), jnp.float32),
            pltpu.VMEM((STEPS, 2, rows_lat, size_z), jnp.float32),
            pltpu.VMEM((STEPS, 2, 2, rows_corner, size_z), jnp.float32),
            pltpu.VMEM((3, size_y, size_z), jnp.int32),
            pltpu.VMEM((1, size_y, size_z), jnp.int32),
            pltpu.VMEM((2, rows_flag, size_z), jnp.int32),
            pltpu.VMEM((2, 8, size_z), jnp.int32),
            pltpu.SemaphoreType.DMA((copies,)),
            pltpu.SemaphoreType.DMA((copies,)),
            pltpu.SemaphoreType.DMA((4,)),
        ],
        compiler_params=pltpu.CompilerParams(collective_id=0, has_side_effects=True),
        name="leapfrog",
    )(displace, velocity, bond_low, bond_high, bc_type)
    return pl.pallas_call(
        advance,
        out_shape=out_shape,
        in_specs=[vmem] * 2,
        out_specs=(vmem, vmem),
        name="advance",
    )(moved, fast)


def solution(mesh):
    cells = P(None, "bar", "lat", None)
    return jax.shard_map(
        functools.partial(local, mesh.shape["bar"], mesh.shape["lat"]),
        mesh=mesh,
        in_specs=(cells, cells, P("bar", "lat", None), P("bar", "lat", None), P()),
        out_specs=(cells, cells),
        check_vma=False,
    )
```
